32 devices in a mesh: part: 2 (over x), data: 4 (over z), stage: 4 (over y, core).
Axes of the slice: x: 2, y: 2, z: 4, core: 2. Of those that a mesh axis runs over, the one named last changes fastest.
Arguments:
- x: bfloat16 [32, 64, 1024], P(('part', 'data')), parts along dimension 0
- g: bfloat16 [32, 64, 1024], P(('part', 'data')), parts along dimension 0
- w_in: bfloat16 [2, 4, 1024, 4096], P(None, 'stage')
- w_out: bfloat16 [2, 4, 4096, 1024], P(None, 'stage')
Outputs:
- output 1: bfloat16 [32, 64, 1024], P(('part', 'data')), parts along dimension 0
- output 2: bfloat16 [32, 64, 1024], P(('part', 'data')), parts along dimension 0
- output 3: float32 [4, 4, 1024, 4096], P('part', 'stage'), parts along dimension 0
- output 4: float32 [4, 4, 4096, 1024], P('part', 'stage'), parts along dimension 0
There are 2 independent parts. The reference program is written for one: setup_inputs(seed, part) draws one part's arguments, and reference() takes and returns one part's arrays. A program takes and returns all parts, laid end to end along the dimension named above; an argument that names none is the same for every part.
All inputs are finite; a program needn't handle non-finite values.
Results may differ from the reference program's by a relative error of at most 0.0176001.
Values are sent between devices in bfloat16 or wider.
A program may use at most 1 GiB of HBM per device.

```python
import functools
import jax
import jax.numpy as jnp
from jax import lax

D_MODEL = 1024
D_FF = 4096
MICRO_TOKENS = 64
ROUNDS = 1
DEVICE_LAYERS = 2
DATA_SIZE = 4
STAGE_SIZE = 4
MICRO_COUNT = ROUNDS * DATA_SIZE * STAGE_SIZE
LAYER_COUNT = DEVICE_LAYERS * STAGE_SIZE


def setup_inputs(seed: int = 0, part: int = 0) -> dict:
    base_key = jax.random.key(seed)
    shared_key, local_key = jax.random.split(base_key)
    local_key = jax.random.fold_in(local_key, part)
    key_in, key_out = jax.random.split(shared_key)
    key_x, key_g = jax.random.split(local_key)
    out_scale = D_FF ** -0.5 * min(0.5, (2.0 / LAYER_COUNT) ** 0.5)
    w_first = jax.random.normal(key_in, (DEVICE_LAYERS, STAGE_SIZE, D_MODEL, D_FF), jnp.float32) * D_MODEL ** -0.5
    w_second = jax.random.normal(key_out, (DEVICE_LAYERS, STAGE_SIZE, D_FF, D_MODEL), jnp.float32) * out_scale
    x_draw = jax.random.normal(key_x, (MICRO_COUNT, MICRO_TOKENS, D_MODEL), jnp.float32)
    g_draw = jax.random.normal(key_g, (MICRO_COUNT, MICRO_TOKENS, D_MODEL), jnp.float32)
    return {'x': x_draw.astype(jnp.bfloat16), 'g': g_draw.astype(jnp.bfloat16), 'w_in': w_first.astype(jnp.bfloat16), 'w_out': w_second.astype(jnp.bfloat16)}


def layer_forward(h_in, w_first, w_second):
    pre_act = jnp.dot(h_in, w_first, preferred_element_type=jnp.float32)
    hidden = jax.nn.gelu(pre_act, approximate=True).astype(jnp.bfloat16)
    delta_out = jnp.dot(hidden, w_second, preferred_element_type=jnp.float32)
    return (h_in.astype(jnp.float32) + delta_out).astype(jnp.bfloat16)


def layer_backward(h_in, w_first, w_second, g_next):
    pre_act = jnp.dot(h_in, w_first, preferred_element_type=jnp.float32)
    gelu_val, gelu_pull = jax.vjp(functools.partial(jax.nn.gelu, approximate=True), pre_act)
    hidden = gelu_val.astype(jnp.bfloat16)
    grad_second = jnp.dot(hidden.T, g_next, preferred_element_type=jnp.float32)
    grad_hidden = jnp.dot(g_next, w_second.T, preferred_element_type=jnp.float32)
    grad_pre = gelu_pull(grad_hidden)[0].astype(jnp.bfloat16)
    grad_first = jnp.dot(h_in.T, grad_pre, preferred_element_type=jnp.float32)
    grad_prev = jnp.dot(grad_pre, w_first.T, preferred_element_type=jnp.float32)
    g_prev = (g_next.astype(jnp.float32) + grad_prev).astype(jnp.bfloat16)
    return g_prev, grad_first, grad_second


def reference(x, g, w_in, w_out):
    first_all = w_in.reshape(LAYER_COUNT, D_MODEL, D_FF)
    second_all = w_out.reshape(LAYER_COUNT, D_FF, D_MODEL)

    def forward_step(h_cur, weights):
        return layer_forward(h_cur, weights[0], weights[1]), h_cur

    def backward_step(g_next, layer_items):
        h_cur, w_first, w_second, acc_first, acc_second = layer_items
        g_prev, grad_first, grad_second = layer_backward(h_cur, w_first, w_second, g_next)
        return g_prev, (acc_first + grad_first, acc_second + grad_second)

    def per_micro(accums, mb_pair):
        x_micro, g_micro = mb_pair
        y_micro, h_saved = lax.scan(forward_step, x_micro, (first_all, second_all))
        dx_micro, new_accums = lax.scan(backward_step, g_micro, (h_saved, first_all, second_all, accums[0], accums[1]), reverse=True)
        return new_accums, (y_micro, dx_micro)

    zero_first = jnp.zeros((LAYER_COUNT, D_MODEL, D_FF), jnp.float32)
    zero_second = jnp.zeros((LAYER_COUNT, D_FF, D_MODEL), jnp.float32)
    accums, results = lax.scan(per_micro, (zero_first, zero_second), (x, g))
    return (results[0], results[1], accums[0].reshape(DEVICE_LAYERS, STAGE_SIZE, D_MODEL, D_FF), accums[1].reshape(DEVICE_LAYERS, STAGE_SIZE, D_FF, D_MODEL))
```

```python
import functools
import math
import jax
import jax.numpy as jnp
from jax import lax
from jax.experimental import pallas as pl
from jax.experimental.pallas import tpu as pltpu
from jax.sharding import PartitionSpec as P

MESH = pl.DeviceIdType.MESH
VMEM_BYTES = 67_000_000
BLOCK_OF = (0, 1, 3, 2)
GELU_K0 = math.sqrt(2.0 / math.pi)
GELU_K1 = GELU_K0 * 0.044715


def gelu_pair(z):
    sq = z * z
    cdf = 0.5 * jnp.tanh(z * (GELU_K0 + GELU_K1 * sq)) + 0.5
    val = z * cdf
    slope = cdf + (val * (1.0 - cdf)) * (2.0 * GELU_K0 + 6.0 * GELU_K1 * sq)
    return val, slope


def chain_kernel(stages, replicas, f_chunk,
                 x_ref, g_ref, w_in_ref, w_out_ref,
                 y_ref, dx_ref, h_out, e_out, a_out, q_out, slope_hbm,
                 h_buf, e_buf, win, wout, slope_buf, a_buf, q_buf, f_send_buf, b_send_buf,
                 w_sem, f_recv, b_recv, f_send, b_send, x_send, g_send,
                 slope_wr, slope_rd, a_wr, q_wr, h_wr, e_wr,
                 y_send, y_loc, y_recv, d_send, d_loc, d_recv):
    stage = lax.axis_index('stage')
    data = lax.axis_index('data')
    rows = x_ref.shape[0]
    fu, bu = rows // 2, rows
    f_per, b_per = 2 * replicas, replicas
    f_units, b_units = 2 * f_per, 2 * b_per
    hidden = win.shape[2]
    is_first = stage == 0
    is_last = stage == stages - 1
    nxt = lax.rem(stage + 1, stages)
    prv = lax.rem(stage + stages - 1, stages)

    def weight_copy(layer, which):
        src, dst = ((w_in_ref, win), (w_out_ref, wout))[which]
        return pltpu.make_async_copy(src.at[layer, 0], dst.at[layer], w_sem.at[layer, which])

    for layer in range(2):
        for which in range(2):
            weight_copy(layer, which).start()

    barrier = pltpu.get_barrier_semaphore()
    for off in range(1, stages):
        pl.semaphore_signal(barrier, inc=1, device_id={'stage': lax.rem(stage + off, stages)}, device_id_type=MESH)
    for off in range(1, replicas):
        pl.semaphore_signal(barrier, inc=1, device_id={'data': lax.rem(data + off, replicas)}, device_id_type=MESH)
    pl.semaphore_wait(barrier, stages + replicas - 2)

    def x_copy(blk, half):
        slot = 2 * blk + half
        return pltpu.make_async_remote_copy(
            src_ref=x_ref.at[pl.ds(half * fu, fu)], dst_ref=h_buf.at[0, pl.ds(slot * fu, fu)],
            send_sem=x_send.at[slot], recv_sem=f_recv.at[slot],
            device_id={'data': lax.rem(data + replicas - BLOCK_OF[blk], replicas)}, device_id_type=MESH)

    def g_copy(blk):
        return pltpu.make_async_remote_copy(
            src_ref=g_ref, dst_ref=e_buf.at[1, pl.ds(blk * bu, bu)],
            send_sem=g_send.at[blk], recv_sem=b_recv.at[blk],
            device_id={'data': lax.rem(data + replicas - BLOCK_OF[blk], replicas)}, device_id_type=MESH)

    @pl.when(is_first)
    def _():
        for half in range(2):
            pltpu.make_async_copy(x_ref.at[pl.ds(half * fu, fu)], h_buf.at[0, pl.ds(half * fu, fu)], f_recv.at[half]).start()
        for blk in range(1, replicas):
            for half in range(2):
                x_copy(blk, half).start()

    @pl.when(is_last)
    def _():
        pltpu.make_async_copy(g_ref, e_buf.at[1, pl.ds(0, bu)], b_recv.at[0]).start()
        for blk in range(1, replicas):
            g_copy(blk).start()

    def f_hop(n):
        v, i = n // f_per, lax.rem(n, f_per)
        slot = lax.rem(n, 2)
        return pltpu.make_async_remote_copy(
            src_ref=f_send_buf.at[slot], dst_ref=h_buf.at[lax.rem(v + is_last.astype(jnp.int32), 2), pl.ds(pl.multiple_of(i * fu, fu), fu)],
            send_sem=f_send.at[slot], recv_sem=f_recv.at[lax.rem(n + f_per * is_last.astype(jnp.int32), f_units)],
            device_id={'stage': nxt}, device_id_type=MESH)

    def y_copies(i):
        src = f_send_buf.at[i]
        dst = y_ref.at[pl.ds(i * fu, fu)]
        remote = [pltpu.make_async_remote_copy(
            src_ref=src, dst_ref=dst, send_sem=y_send.at[i, k], recv_sem=y_recv.at[i],
            device_id={'stage': k}, device_id_type=MESH) for k in range(stages - 1)]
        return remote, pltpu.make_async_copy(src, dst, y_loc.at[i])

    def slope_write(n):
        v, i = n // f_per, lax.rem(n, f_per)
        slot = lax.rem(n, 2)
        return pltpu.make_async_copy(
            slope_buf.at[pl.ds(pl.multiple_of(bu + slot * fu, fu), fu)],
            slope_hbm.at[v, pl.ds(pl.multiple_of(i * fu, fu), fu)], slope_wr.at[slot])

    def a_write(n):
        v, i = n // f_per, lax.rem(n, f_per)
        slot = lax.rem(n, 2)
        return pltpu.make_async_copy(a_buf.at[slot], a_out.at[v, pl.ds(pl.multiple_of(i * fu, fu), fu)], a_wr.at[slot])

    def hops(n):
        return jnp.logical_not(jnp.logical_and(is_last, n >= f_per))

    def f_step(n, carry):
        v, i = n // f_per, lax.rem(n, f_per)
        slot = lax.rem(n, 2)
        row0 = pl.multiple_of(i * fu, fu)

        @pl.when(i == 0)
        def _():
            pltpu.make_async_copy(w_in_ref.at[v, 0], win.at[v], w_sem.at[v, 0]).wait()
            pltpu.make_async_copy(w_out_ref.at[v, 0], wout.at[v], w_sem.at[v, 1]).wait()

        @pl.when(n >= 2)
        def _():
            slope_write(n - 2).wait()
            a_write(n - 2).wait()

        pltpu.make_async_copy(x_ref.at[pl.ds(0, fu)], h_buf.at[v, pl.ds(row0, fu)], f_recv.at[n]).wait()
        h_in = h_buf[v, pl.ds(row0, fu), :]
        for c in range(hidden // f_chunk):
            cols = pl.ds(c * f_chunk, f_chunk)
            z = jnp.dot(h_in, win[v, :, cols], preferred_element_type=jnp.float32)
            val, slope = gelu_pair(z)
            slope_buf[pl.ds(pl.multiple_of(bu + slot * fu, fu), fu), cols] = slope
            a_buf[slot, :, cols] = val.astype(jnp.bfloat16)
        slope_write(n).start()
        a_write(n).start()

        @pl.when(jnp.logical_and(n >= 2, hops(n - 2)))
        def _():
            f_hop(n - 2).wait_send()

        @pl.when(jnp.logical_or(hops(n), i < 2))
        def _():
            delta = jnp.dot(a_buf[slot], wout[v], preferred_element_type=jnp.float32)
            f_send_buf[slot] = (h_buf[v, pl.ds(row0, fu), :].astype(jnp.float32) + delta).astype(jnp.bfloat16)

        @pl.when(hops(n))
        def _():
            f_hop(n).start()

        for k in range(2):
            @pl.when(jnp.logical_and(is_last, n == f_per + k))
            def _():
                remote, local = y_copies(k)
                for copy in remote:
                    copy.start()
                local.start()
        return carry

    lax.fori_loop(0, f_units, f_step, 0)
    for k in range(2):
        n = f_units - 2 + k
        slope_write(n).wait()
        a_write(n).wait()

    @pl.when(jnp.logical_not(is_last))
    def _():
        for k in range(2):
            f_hop(f_units - 2 + k).wait_send()

    def h_copy(layer):
        return pltpu.make_async_copy(h_buf.at[layer], h_out.at[layer], h_wr.at[layer])

    def e_copy(layer):
        return pltpu.make_async_copy(e_buf.at[layer], e_out.at[layer], e_wr.at[layer])

    for layer in range(2):
        h_copy(layer).start()

    def slope_read(n):
        v, j = 1 - n // b_per, lax.rem(n, b_per)
        slot = lax.rem(n, 2)
        return pltpu.make_async_copy(
            slope_hbm.at[v, pl.ds(pl.multiple_of(j * bu, bu), bu)],
            slope_buf.at[pl.ds(pl.multiple_of(slot * bu, bu), bu)], slope_rd.at[slot])

    def q_write(n):
        v, j = 1 - n // b_per, lax.rem(n, b_per)
        slot = lax.rem(n, 2)
        return pltpu.make_async_copy(q_buf.at[slot], q_out.at[v, pl.ds(pl.multiple_of(j * bu, bu), bu)], q_wr.at[slot])

    def b_hop(n):
        v, j = 1 - n // b_per, lax.rem(n, b_per)
        slot = lax.rem(n, 2)
        wrap = is_first.astype(jnp.int32)
        return pltpu.make_async_remote_copy(
            src_ref=b_send_buf.at[slot], dst_ref=e_buf.at[lax.rem(v + wrap, 2), pl.ds(pl.multiple_of(j * bu, bu), bu)],
            send_sem=b_send.at[slot], recv_sem=b_recv.at[lax.rem(n + b_per * wrap, b_units)],
            device_id={'stage': prv}, device_id_type=MESH)

    def d_copies():
        src = b_send_buf.at[0]
        remote = [pltpu.make_async_remote_copy(
            src_ref=src, dst_ref=dx_ref, send_sem=d_send.at[k - 1], recv_sem=d_recv.at[0],
            device_id={'stage': k}, device_id_type=MESH) for k in range(1, stages)]
        return remote, pltpu.make_async_copy(src, dx_ref, d_loc.at[0])

    def b_hops(n):
        return jnp.logical_not(jnp.logical_and(is_first, n >= b_per))

    for n in range(2):
        slope_read(n).start()

    def b_step(n, carry):
        v, j = 1 - n // b_per, lax.rem(n, b_per)
        slot = lax.rem(n, 2)
        row0 = pl.multiple_of(j * bu, bu)
        slope_read(n).wait()

        @pl.when(n >= 2)
        def _():
            q_write(n - 2).wait()

        pltpu.make_async_copy(g_ref, e_buf.at[v, pl.ds(row0, bu)], b_recv.at[n]).wait()
        e_in = e_buf[v, pl.ds(row0, bu), :]
        for c in range(hidden // f_chunk):
            cols = pl.ds(c * f_chunk, f_chunk)
            d_act = lax.dot_general(e_in, wout[v, cols, :], (((1,), (1,)), ((), ())), preferred_element_type=jnp.float32)
            slope = slope_buf[pl.ds(pl.multiple_of(slot * bu, bu), bu), cols]
            q_buf[slot, :, cols] = (slope * d_act).astype(jnp.bfloat16)
        q_write(n).start()

        @pl.when(n + 2 < b_units)
        def _():
            slope_read(n + 2).start()

        @pl.when(jnp.logical_and(n >= 2, b_hops(n - 2)))
        def _():
            b_hop(n - 2).wait_send()

        @pl.when(jnp.logical_or(b_hops(n), j == 0))
        def _():
            delta = lax.dot_general(q_buf[slot], win[v], (((1,), (1,)), ((), ())), preferred_element_type=jnp.float32)
            b_send_buf[slot] = (e_buf[v, pl.ds(row0, bu), :].astype(jnp.float32) + delta).astype(jnp.bfloat16)

        @pl.when(b_hops(n))
        def _():
            b_hop(n).start()

        @pl.when(jnp.logical_and(is_first, n == b_per))
        def _():
            remote, local = d_copies()
            for copy in remote:
                copy.start()
            local.start()
        return carry

    @pl.when(is_last)
    def _():
        for k in range(2):
            remote, local = y_copies(k)
            for copy in remote:
                copy.wait_send()
            local.wait()

    lax.fori_loop(0, b_units, b_step, 0)
    for layer in range(2):
        e_copy(layer).start()
    for k in range(2):
        q_write(b_units - 2 + k).wait()

    @pl.when(jnp.logical_not(is_first))
    def _():
        for k in range(2):
            b_hop(b_units - 2 + k).wait_send()
        pltpu.make_async_copy(b_send_buf.at[0], dx_ref, d_recv.at[0]).wait()

    @pl.when(is_first)
    def _():
        remote, local = d_copies()
        for copy in remote:
            copy.wait_send()
        local.wait()
        for blk in range(1, replicas):
            for half in range(2):
                x_copy(blk, half).wait_send()

    @pl.when(jnp.logical_not(is_last))
    def _():
        for k in range(2):
            pltpu.make_async_copy(f_send_buf.at[k], y_ref.at[pl.ds(k * fu, fu)], y_recv.at[k]).wait()

    @pl.when(is_last)
    def _():
        for blk in range(1, replicas):
            g_copy(blk).wait_send()

    for layer in range(2):
        h_copy(layer).wait()
        e_copy(layer).wait()


def run_chain(x, g, w_in, w_out, stages, replicas):
    rows, model = x.shape
    hidden = w_in.shape[-1]
    total = rows * replicas
    fu, bu = rows // 2, rows
    f_chunk = hidden // 4
    any_spec = pl.BlockSpec(memory_space=pl.ANY)
    bf, f32 = jnp.bfloat16, jnp.float32
    dma = pltpu.SemaphoreType.DMA
    shape = jax.ShapeDtypeStruct
    f_units, b_units = 4 * replicas, 2 * replicas
    return pl.pallas_call(
        functools.partial(chain_kernel, stages, replicas, f_chunk),
        out_shape=(shape((rows, model), bf), shape((rows, model), bf),
                   shape((2, total, model), bf), shape((2, total, model), bf),
                   shape((2, total, hidden), bf), shape((2, total, hidden), bf),
                   shape((2, total, hidden), f32)),
        in_specs=[any_spec] * 4,
        out_specs=(any_spec,) * 7,
        scratch_shapes=[
            pltpu.VMEM((2, total, model), bf), pltpu.VMEM((2, total, model), bf),
            pltpu.VMEM((2, model, hidden), bf), pltpu.VMEM((2, hidden, model), bf),
            pltpu.VMEM((2 * bu, hidden), f32), pltpu.VMEM((2, fu, hidden), bf), pltpu.VMEM((2, bu, hidden), bf),
            pltpu.VMEM((2, fu, model), bf), pltpu.VMEM((2, bu, model), bf),
            dma((2, 2)), dma((f_units,)), dma((b_units,)), dma((2,)), dma((2,)), dma((2 * replicas,)), dma((replicas,)),
            dma((2,)), dma((2,)), dma((2,)), dma((2,)), dma((2,)), dma((2,)),
            dma((2, stages - 1)), dma((2,)), dma((2,)), dma((stages - 1,)), dma((1,)), dma((1,)),
        ],
        compiler_params=pltpu.CompilerParams(collective_id=0, has_side_effects=True, vmem_limit_bytes=VMEM_BYTES),
        name='chain',
    )(x, g, w_in, w_out)


def solution(mesh):
    stages = mesh.shape['stage']
    replicas = mesh.shape['data']

    def local_fn(x, g, w_in, w_out):
        micro, tokens, model = x.shape
        y, dx, h_all, e_all, a_all, q_all, _ = run_chain(
            x.reshape(micro * tokens, model), g.reshape(micro * tokens, model), w_in, w_out, stages, replicas)
        grad_first = jnp.einsum('vtd,vtf->vdf', h_all, q_all, preferred_element_type=jnp.float32)
        grad_second = jnp.einsum('vtf,vtd->vfd', a_all, e_all, preferred_element_type=jnp.float32)
        return y.reshape(x.shape), dx.reshape(x.shape), grad_first[:, None], grad_second[:, None]

    spec_rows = P(('part', 'data'))
    spec_weights = P(None, 'stage')
    spec_grads = P('part', 'stage')
    return jax.shard_map(local_fn, mesh=mesh, in_specs=(spec_rows, spec_rows, spec_weights, spec_weights), out_specs=(spec_rows, spec_rows, spec_grads, spec_grads), check_vma=False)
```

```python
import functools
import math
import jax
import jax.numpy as jnp
from jax import lax
from jax.experimental import pallas as pl
from jax.experimental.pallas import tpu as pltpu
from jax.sharding import PartitionSpec as P

MESH = pl.DeviceIdType.MESH
VMEM_BYTES = 67_000_000
BLOCK_OF = (0, 1, 3, 2)
GELU_K0 = math.sqrt(2.0 / math.pi)
GELU_K1 = GELU_K0 * 0.044715


def gelu_pair(z):
    sq = z * z
    cdf = 0.5 * jnp.tanh(z * (GELU_K0 + GELU_K1 * sq)) + 0.5
    val = z * cdf
    slope = cdf + (val * (1.0 - cdf)) * (2.0 * GELU_K0 + 6.0 * GELU_K1 * sq)
    return val, slope


def chain_kernel(stages, replicas, f_chunk,
                 x_ref, g_ref, w_in_ref, w_out_ref,
                 y_ref, dx_ref, h_out, e_out, a_out, q_out, slope_hbm, wide_hbm, tall_hbm,
                 h_buf, e_buf, wide, tall, slope_buf, a_buf, q_buf, f_send_buf, b_send_buf, wide_stage, tall_stage,
                 w_sem, wt_wr, wt_rd, f_recv, b_recv, f_send, b_send, x_send, g_send,
                 slope_wr, slope_rd, a_wr, q_wr, h_wr, e_wr,
                 y_send, y_loc, y_recv, d_send, d_loc, d_recv):
    stage = lax.axis_index('stage')
    data = lax.axis_index('data')
    unit = x_ref.shape[0] // 2
    per = 2 * replicas
    hidden = wide.shape[2]
    part_f = hidden // per
    is_first = stage == 0
    is_last = stage == stages - 1
    nxt = lax.rem(stage + 1, stages)
    prv = lax.rem(stage + stages - 1, stages)

    def rows_of(i):
        return pl.ds(pl.multiple_of(i * unit, unit), unit)

    def weight_copies(layer):
        return (pltpu.make_async_copy(w_in_ref.at[layer, 0], wide.at[layer], w_sem.at[layer, 0]),
                pltpu.make_async_copy(w_out_ref.at[layer, 0], tall.at[layer], w_sem.at[layer, 1]))

    for layer in range(2):
        for copy in weight_copies(layer):
            copy.start()

    barrier = pltpu.get_barrier_semaphore()
    for off in range(1, stages):
        pl.semaphore_signal(barrier, inc=1, device_id={'stage': lax.rem(stage + off, stages)}, device_id_type=MESH)
    for off in range(1, replicas):
        pl.semaphore_signal(barrier, inc=1, device_id={'data': lax.rem(data + off, replicas)}, device_id_type=MESH)
    pl.semaphore_wait(barrier, stages + replicas - 2)

    def share_copy(src, dst, send_sem, recv_sem, blk, half):
        slot = 2 * blk + half
        return pltpu.make_async_remote_copy(
            src_ref=src.at[pl.ds(half * unit, unit)], dst_ref=dst.at[pl.ds(slot * unit, unit)],
            send_sem=send_sem.at[slot], recv_sem=recv_sem.at[slot],
            device_id={'data': lax.rem(data + replicas - BLOCK_OF[blk], replicas)}, device_id_type=MESH)

    def share(src, dst, send_sem, recv_sem):
        for half in range(2):
            rows = pl.ds(half * unit, unit)
            pltpu.make_async_copy(src.at[rows], dst.at[rows], recv_sem.at[half]).start()
        for blk in range(1, replicas):
            for half in range(2):
                share_copy(src, dst, send_sem, recv_sem, blk, half).start()

    @pl.when(is_first)
    def _():
        share(x_ref, h_buf.at[0], x_send, f_recv)

    @pl.when(is_last)
    def _():
        share(g_ref, e_buf.at[1], g_send, b_recv)

    def f_hop(v, i):
        slot = lax.rem(i, 2)
        last = is_last.astype(jnp.int32)
        return pltpu.make_async_remote_copy(
            src_ref=f_send_buf.at[slot], dst_ref=h_buf.at[lax.rem(v + last, 2), rows_of(i)],
            send_sem=f_send.at[slot], recv_sem=f_recv.at[lax.rem(v * per + i + per * last, 2 * per)],
            device_id={'stage': nxt}, device_id_type=MESH)

    def y_copies(i):
        src = f_send_buf.at[i]
        dst = y_ref.at[pl.ds(i * unit, unit)]
        remote = [pltpu.make_async_remote_copy(
            src_ref=src, dst_ref=dst, send_sem=y_send.at[i, k], recv_sem=y_recv.at[i],
            device_id={'stage': k}, device_id_type=MESH) for k in range(stages - 1)]
        return remote, pltpu.make_async_copy(src, dst, y_loc.at[i])

    def f_writes(v, i):
        slot = lax.rem(i, 2)
        return (pltpu.make_async_copy(slope_buf.at[rows_of(2 + slot)], slope_hbm.at[v, rows_of(i)], slope_wr.at[slot]),
                pltpu.make_async_copy(a_buf.at[slot], a_out.at[v, rows_of(i)], a_wr.at[slot]))

    def wt_writes(i):
        slot = lax.rem(i, 2)
        return (pltpu.make_async_copy(wide_stage.at[slot], wide_hbm.at[:, pl.ds(pl.multiple_of(i * part_f, part_f), part_f)], wt_wr.at[slot, 0]),
                pltpu.make_async_copy(tall_stage.at[slot], tall_hbm.at[pl.ds(pl.multiple_of(i * part_f, part_f), part_f)], wt_wr.at[slot, 1]))

    def f_compute(v, i, full):
        slot = lax.rem(i, 2)
        h_in = h_buf[v, rows_of(i), :]
        for c in range(hidden // f_chunk):
            cols = pl.ds(c * f_chunk, f_chunk)
            z = jnp.dot(h_in, wide[v, :, cols], preferred_element_type=jnp.float32)
            val, slope = gelu_pair(z)
            slope_buf[rows_of(2 + slot), cols] = slope
            a_buf[slot, :, cols] = val.astype(jnp.bfloat16)
        strip = pl.ds(pl.multiple_of(i * part_f, part_f), part_f)
        if v == 0:
            wide_stage[slot] = tall[v, strip, :].T
            tall_stage[slot] = wide[v, :, strip].T
        else:
            wide[0, :, strip] = tall[v, strip, :].T
            tall[0, strip, :] = wide[v, :, strip].T
        if full:
            delta = jnp.dot(a_buf[slot], tall[v], preferred_element_type=jnp.float32)
            f_send_buf[slot] = (h_in.astype(jnp.float32) + delta).astype(jnp.bfloat16)

    def f_wait(v, i):
        pltpu.make_async_copy(x_ref.at[pl.ds(0, unit)], h_buf.at[v, rows_of(i)], f_recv.at[v * per + i]).wait()

    for copy in weight_copies(0):
        copy.wait()

    def f_step_0(i, carry):
        @pl.when(i >= 2)
        def _():
            for copy in f_writes(0, i - 2) + wt_writes(i - 2):
                copy.wait()
            f_hop(0, i - 2).wait_send()

        f_wait(0, i)
        f_compute(0, i, True)
        f_hop(0, i).start()
        for copy in f_writes(0, i) + wt_writes(i):
            copy.start()
        return carry

    lax.fori_loop(0, per, f_step_0, 0)
    for copy in weight_copies(1):
        copy.wait()
    for i in range(per - 2, per):
        f_hop(0, i).wait_send()

    def slope_read(v, j):
        slot = lax.rem(j, 2)
        return pltpu.make_async_copy(slope_hbm.at[v, rows_of(j)], slope_buf.at[rows_of(slot)], slope_rd.at[slot])

    def f_step_1(i, carry):
        @pl.when(i < 2)
        def _():
            for copy in f_writes(0, per - 2 + i) + wt_writes(per - 2 + i):
                copy.wait()

        @pl.when(i >= 2)
        def _():
            for copy in f_writes(1, i - 2):
                copy.wait()

        for j in range(2):
            @pl.when(i == 2 + j)
            def _():
                slope_read(1, j).start()

        @pl.when(jnp.logical_and(i >= 2, jnp.logical_not(is_last)))
        def _():
            f_hop(1, i - 2).wait_send()

        f_wait(1, i)

        @pl.when(jnp.logical_or(jnp.logical_not(is_last), i < 2))
        def _():
            f_compute(1, i, True)

        @pl.when(jnp.logical_and(is_last, i >= 2))
        def _():
            f_compute(1, i, False)

        @pl.when(jnp.logical_not(is_last))
        def _():
            f_hop(1, i).start()

        for copy in f_writes(1, i):
            copy.start()
        for k in range(2):
            @pl.when(jnp.logical_and(is_last, i == k))
            def _():
                remote, local = y_copies(k)
                for copy in remote:
                    copy.start()
                local.start()
        return carry

    lax.fori_loop(0, per, f_step_1, 0)

    def wt_reads():
        return (pltpu.make_async_copy(wide_hbm, wide.at[1], wt_rd.at[0]),
                pltpu.make_async_copy(tall_hbm, tall.at[1], wt_rd.at[1]))

    def h_copy(layer):
        return pltpu.make_async_copy(h_buf.at[layer], h_out.at[layer], h_wr.at[layer])

    def e_copy(layer):
        return pltpu.make_async_copy(e_buf.at[layer], e_out.at[layer], e_wr.at[layer])

    def q_write(v, j):
        slot = lax.rem(j, 2)
        return pltpu.make_async_copy(q_buf.at[slot], q_out.at[v, rows_of(j)], q_wr.at[slot])

    def b_hop(v, j):
        slot = lax.rem(j, 2)
        wrap = is_first.astype(jnp.int32)
        return pltpu.make_async_remote_copy(
            src_ref=b_send_buf.at[slot], dst_ref=e_buf.at[lax.rem(v + wrap, 2), rows_of(j)],
            send_sem=b_send.at[slot], recv_sem=b_recv.at[lax.rem((1 - v) * per + j + per * wrap, 2 * per)],
            device_id={'stage': prv}, device_id_type=MESH)

    def d_copies(i):
        src = b_send_buf.at[i]
        dst = dx_ref.at[pl.ds(i * unit, unit)]
        remote = [pltpu.make_async_remote_copy(
            src_ref=src, dst_ref=dst, send_sem=d_send.at[i, k - 1], recv_sem=d_recv.at[i],
            device_id={'stage': k}, device_id_type=MESH) for k in range(1, stages)]
        return remote, pltpu.make_async_copy(src, dst, d_loc.at[i])

    def hops(v):
        return jnp.logical_not(jnp.logical_and(is_first, v == 0))

    for copy in wt_reads():
        copy.start()

    def b_compute(v, j, full):
        slot = lax.rem(j, 2)
        e_in = e_buf[v, rows_of(j), :]
        for c in range(hidden // f_chunk):
            cols = pl.ds(c * f_chunk, f_chunk)
            d_act = jnp.dot(e_in, wide[1 - v, :, cols], preferred_element_type=jnp.float32)
            q_buf[slot, :, cols] = (slope_buf[rows_of(slot), cols] * d_act).astype(jnp.bfloat16)
        if full:
            delta = jnp.dot(q_buf[slot], tall[1 - v], preferred_element_type=jnp.float32)
            b_send_buf[slot] = (e_in.astype(jnp.float32) + delta).astype(jnp.bfloat16)

    def b_step(n, carry):
        v, j = 1 - n // per, lax.rem(n, per)
        slope_read(v, j).wait()

        @pl.when(n == 1)
        def _():
            for i in range(per - 2, per):
                for copy in f_writes(1, i):
                    copy.wait()
            for layer in range(2):
                h_copy(layer).start()

        @pl.when(n == per)
        def _():
            for copy in wt_reads():
                copy.wait()
            e_copy(1).start()

        @pl.when(n >= 2)
        def _():
            back = n - 2
            q_write(1 - back // per, lax.rem(back, per)).wait()

        @pl.when(jnp.logical_and(n >= 2, hops(1 - (n - 2) // per)))
        def _():
            b_hop(1 - (n - 2) // per, lax.rem(n - 2, per)).wait_send()

        pltpu.make_async_copy(x_ref.at[pl.ds(0, unit)], e_buf.at[v, rows_of(j)], b_recv.at[n]).wait()

        @pl.when(jnp.logical_or(hops(v), j < 2))
        def _():
            b_compute(v, j, True)

        @pl.when(jnp.logical_not(jnp.logical_or(hops(v), j < 2)))
        def _():
            b_compute(v, j, False)

        @pl.when(hops(v))
        def _():
            b_hop(v, j).start()

        q_write(v, j).start()

        @pl.when(n + 2 < 2 * per)
        def _():
            ahead = n + 2
            slope_read(1 - ahead // per, lax.rem(ahead, per)).start()

        for k in range(2):
            @pl.when(jnp.logical_and(is_first, n == per + k))
            def _():
                remote, local = d_copies(k)
                for copy in remote:
                    copy.start()
                local.start()
        return carry

    lax.fori_loop(0, 2 * per, b_step, 0)
    e_copy(0).start()
    for j in range(per - 2, per):
        q_write(0, j).wait()

    def share_done(src, dst, send_sem, recv_sem):
        for blk in range(1, replicas):
            for half in range(2):
                share_copy(src, dst, send_sem, recv_sem, blk, half).wait_send()

    @pl.when(is_first)
    def _():
        for k in range(2):
            remote, local = d_copies(k)
            for copy in remote:
                copy.wait_send()
            local.wait()
        share_done(x_ref, h_buf.at[0], x_send, f_recv)

    @pl.when(jnp.logical_not(is_first))
    def _():
        for j in range(per - 2, per):
            b_hop(0, j).wait_send()
        for k in range(2):
            pltpu.make_async_copy(b_send_buf.at[k], dx_ref.at[pl.ds(k * unit, unit)], d_recv.at[k]).wait()

    @pl.when(is_last)
    def _():
        for k in range(2):
            remote, local = y_copies(k)
            for copy in remote:
                copy.wait_send()
            local.wait()
        share_done(g_ref, e_buf.at[1], g_send, b_recv)

    @pl.when(jnp.logical_not(is_last))
    def _():
        for i in range(per - 2, per):
            f_hop(1, i).wait_send()
        for k in range(2):
            pltpu.make_async_copy(f_send_buf.at[k], y_ref.at[pl.ds(k * unit, unit)], y_recv.at[k]).wait()

    for layer in range(2):
        h_copy(layer).wait()
        e_copy(layer).wait()


def run_chain(x, g, w_in, w_out, stages, replicas):
    rows, model = x.shape
    hidden = w_in.shape[-1]
    total = rows * replicas
    unit, per = rows // 2, 2 * replicas
    f_chunk = hidden // 4
    part_f = hidden // per
    any_spec = pl.BlockSpec(memory_space=pl.ANY)
    bf, f32 = jnp.bfloat16, jnp.float32
    dma = pltpu.SemaphoreType.DMA
    shape = jax.ShapeDtypeStruct
    return pl.pallas_call(
        functools.partial(chain_kernel, stages, replicas, f_chunk),
        out_shape=(shape((rows, model), bf), shape((rows, model), bf),
                   shape((2, total, model), bf), shape((2, total, model), bf),
                   shape((2, total, hidden), bf), shape((2, total, hidden), bf),
                   shape((2, total, hidden), f32), shape((model, hidden), bf), shape((hidden, model), bf)),
        in_specs=[any_spec] * 4,
        out_specs=(any_spec,) * 9,
        scratch_shapes=[
            pltpu.VMEM((2, total, model), bf), pltpu.VMEM((2, total, model), bf),
            pltpu.VMEM((2, model, hidden), bf), pltpu.VMEM((2, hidden, model), bf),
            pltpu.VMEM((4 * unit, hidden), f32), pltpu.VMEM((2, unit, hidden), bf), pltpu.VMEM((2, unit, hidden), bf),
            pltpu.VMEM((2, unit, model), bf), pltpu.VMEM((2, unit, model), bf),
            pltpu.VMEM((2, model, part_f), bf), pltpu.VMEM((2, part_f, model), bf),
            dma((2, 2)), dma((2, 2)), dma((2,)), dma((2 * per,)), dma((2 * per,)), dma((2,)), dma((2,)), dma((per,)), dma((per,)),
            dma((2,)), dma((2,)), dma((2,)), dma((2,)), dma((2,)), dma((2,)),
            dma((2, stages - 1)), dma((2,)), dma((2,)), dma((2, stages - 1)), dma((2,)), dma((2,)),
        ],
        compiler_params=pltpu.CompilerParams(collective_id=0, has_side_effects=True, vmem_limit_bytes=VMEM_BYTES),
        name='chain',
    )(x, g, w_in, w_out)


def solution(mesh):
    stages = mesh.shape['stage']
    replicas = mesh.shape['data']

    def local_fn(x, g, w_in, w_out):
        micro, tokens, model = x.shape
        y, dx, h_all, e_all, a_all, q_all, *_ = run_chain(
            x.reshape(micro * tokens, model), g.reshape(micro * tokens, model), w_in, w_out, stages, replicas)
        grad_first = jnp.einsum('vtd,vtf->vdf', h_all, q_all, preferred_element_type=jnp.float32)
        grad_second = jnp.einsum('vtf,vtd->vfd', a_all, e_all, preferred_element_type=jnp.float32)
        return y.reshape(x.shape), dx.reshape(x.shape), grad_first[:, None], grad_second[:, None]

    spec_rows = P(('part', 'data'))
    spec_weights = P(None, 'stage')
    spec_grads = P('part', 'stage')
    return jax.shard_map(local_fn, mesh=mesh, in_specs=(spec_rows, spec_rows, spec_weights, spec_weights), out_specs=(spec_rows, spec_rows, spec_grads, spec_grads), check_vma=False)
```

```python
import functools
import math
import jax
import jax.numpy as jnp
from jax import lax
from jax.experimental import pallas as pl
from jax.experimental.pallas import tpu as pltpu
from jax.sharding import PartitionSpec as P

MESH = pl.DeviceIdType.MESH
VMEM_BYTES = 67_000_000
BLOCK_OF = (0, 1, 3, 2)
GELU_K0 = math.sqrt(2.0 / math.pi)
GELU_K1 = GELU_K0 * 0.044715


def gelu_pair(z):
    sq = z * z
    cdf = 0.5 * jnp.tanh(z * (GELU_K0 + GELU_K1 * sq)) + 0.5
    val = z * cdf
    slope = cdf + (val * (1.0 - cdf)) * (2.0 * GELU_K0 + 6.0 * GELU_K1 * sq)
    return val, slope


def chain_kernel(stages, replicas, f_chunk,
                 x_ref, g_ref, w_in_ref, w_out_ref,
                 y_ref, dx_ref, ht_out, e_out, at_out, q_out, a_hbm, slope_hbm, wide_hbm, tall_hbm,
                 h_buf, e_buf, wide, tall, slope_buf, a_buf, a_back, q_buf, f_send_buf, b_send_buf, wide_stage, tall_stage,
                 w_sem, wt_wr, wt_rd, f_recv, b_recv, f_send, b_send, x_send, g_send,
                 slope_wr, slope_rd, a_wr, a_rd, q_wr, ht_wr, at_wr, e_wr,
                 y_send, y_loc, y_recv, d_send, d_loc, d_recv):
    stage = lax.axis_index('stage')
    data = lax.axis_index('data')
    unit = x_ref.shape[0] // 2
    per = 2 * replicas
    hidden = wide.shape[2]
    part_f = hidden // per
    is_first = stage == 0
    is_last = stage == stages - 1
    nxt = lax.rem(stage + 1, stages)
    prv = lax.rem(stage + stages - 1, stages)

    def rows_of(i):
        return pl.ds(pl.multiple_of(i * unit, unit), unit)

    def weight_copies(layer):
        return (pltpu.make_async_copy(w_in_ref.at[layer, 0], wide.at[layer], w_sem.at[layer, 0]),
                pltpu.make_async_copy(w_out_ref.at[layer, 0], tall.at[layer], w_sem.at[layer, 1]))

    for copy in weight_copies(0):
        copy.start()

    barrier = pltpu.get_barrier_semaphore()
    for off in range(1, stages):
        pl.semaphore_signal(barrier, inc=1, device_id={'stage': lax.rem(stage + off, stages)}, device_id_type=MESH)
    for off in range(1, replicas):
        pl.semaphore_signal(barrier, inc=1, device_id={'data': lax.rem(data + off, replicas)}, device_id_type=MESH)
    pl.semaphore_wait(barrier, stages + replicas - 2)

    def share_copy(src, dst, send_sem, recv_sem, blk, half):
        slot = 2 * blk + half
        return pltpu.make_async_remote_copy(
            src_ref=src.at[pl.ds(half * unit, unit)], dst_ref=dst.at[pl.ds(slot * unit, unit)],
            send_sem=send_sem.at[slot], recv_sem=recv_sem.at[slot],
            device_id={'data': lax.rem(data + replicas - BLOCK_OF[blk], replicas)}, device_id_type=MESH)

    def share(src, dst, send_sem, recv_sem):
        for half in range(2):
            rows = pl.ds(half * unit, unit)
            pltpu.make_async_copy(src.at[rows], dst.at[rows], recv_sem.at[half]).start()
        for blk in range(1, replicas):
            for half in range(2):
                share_copy(src, dst, send_sem, recv_sem, blk, half).start()

    @pl.when(is_first)
    def _():
        share(x_ref, h_buf.at[0], x_send, f_recv)

    @pl.when(is_last)
    def _():
        share(g_ref, e_buf.at[1], g_send, b_recv)

    def f_hop(v, i):
        slot = lax.rem(i, 2)
        last = is_last.astype(jnp.int32)
        return pltpu.make_async_remote_copy(
            src_ref=f_send_buf.at[slot], dst_ref=h_buf.at[lax.rem(v + last, 2), rows_of(i)],
            send_sem=f_send.at[slot], recv_sem=f_recv.at[lax.rem(v * per + i + per * last, 2 * per)],
            device_id={'stage': nxt}, device_id_type=MESH)

    def y_copies(i):
        src = f_send_buf.at[i]
        dst = y_ref.at[pl.ds(i * unit, unit)]
        remote = [pltpu.make_async_remote_copy(
            src_ref=src, dst_ref=dst, send_sem=y_send.at[i, k], recv_sem=y_recv.at[i],
            device_id={'stage': k}, device_id_type=MESH) for k in range(stages - 1)]
        return remote, pltpu.make_async_copy(src, dst, y_loc.at[i])

    def f_writes(v, i):
        slot = lax.rem(i, 2)
        return (pltpu.make_async_copy(slope_buf.at[rows_of(2 + slot)], slope_hbm.at[v, rows_of(i)], slope_wr.at[slot]),
                pltpu.make_async_copy(a_buf.at[slot], a_hbm.at[v, rows_of(i)], a_wr.at[slot]))

    def wt_writes(i):
        slot = lax.rem(i, 2)
        return (pltpu.make_async_copy(wide_stage.at[slot], wide_hbm.at[:, pl.ds(pl.multiple_of(i * part_f, part_f), part_f)], wt_wr.at[slot, 0]),
                pltpu.make_async_copy(tall_stage.at[slot], tall_hbm.at[pl.ds(pl.multiple_of(i * part_f, part_f), part_f)], wt_wr.at[slot, 1]))

    def f_compute(v, i, full):
        slot = lax.rem(i, 2)
        h_in = h_buf[v, rows_of(i), :]
        for c in range(hidden // f_chunk):
            cols = pl.ds(c * f_chunk, f_chunk)
            z = jnp.dot(h_in, wide[v, :, cols], preferred_element_type=jnp.float32)
            val, slope = gelu_pair(z)
            slope_buf[rows_of(2 + slot), cols] = slope
            a_buf[slot, :, cols] = val.astype(jnp.bfloat16)
        strip = pl.ds(pl.multiple_of(i * part_f, part_f), part_f)
        if v == 0:
            wide_stage[slot] = tall[v, strip, :].T
            tall_stage[slot] = wide[v, :, strip].T
        else:
            wide[0, :, strip] = tall[v, strip, :].T
            tall[0, strip, :] = wide[v, :, strip].T
        if full:
            delta = jnp.dot(a_buf[slot], tall[v], preferred_element_type=jnp.float32)
            f_send_buf[slot] = (h_in.astype(jnp.float32) + delta).astype(jnp.bfloat16)

    def f_wait(v, i):
        pltpu.make_async_copy(x_ref.at[pl.ds(0, unit)], h_buf.at[v, rows_of(i)], f_recv.at[v * per + i]).wait()

    for copy in weight_copies(0):
        copy.wait()
    for copy in weight_copies(1):
        copy.start()

    def f_step_0(i, carry):
        @pl.when(i >= 2)
        def _():
            for copy in f_writes(0, i - 2) + wt_writes(i - 2):
                copy.wait()
            f_hop(0, i - 2).wait_send()

        f_wait(0, i)
        f_compute(0, i, True)
        f_hop(0, i).start()
        for copy in f_writes(0, i) + wt_writes(i):
            copy.start()
        return carry

    lax.fori_loop(0, per, f_step_0, 0)
    for copy in weight_copies(1):
        copy.wait()
    for i in range(per - 2, per):
        f_hop(0, i).wait_send()

    def b_reads(v, j):
        slot = lax.rem(j, 2)
        return (pltpu.make_async_copy(slope_hbm.at[v, rows_of(j)], slope_buf.at[rows_of(slot)], slope_rd.at[slot]),
                pltpu.make_async_copy(a_hbm.at[v, rows_of(j)], a_back.at[slot], a_rd.at[slot]))

    def f_step_1(i, carry):
        @pl.when(i < 2)
        def _():
            for copy in f_writes(0, per - 2 + i) + wt_writes(per - 2 + i):
                copy.wait()

        @pl.when(i >= 2)
        def _():
            for copy in f_writes(1, i - 2):
                copy.wait()

        for j in range(2):
            @pl.when(i == 2 + j)
            def _():
                for copy in b_reads(1, j):
                    copy.start()

        @pl.when(jnp.logical_and(i >= 2, jnp.logical_not(is_last)))
        def _():
            f_hop(1, i - 2).wait_send()

        f_wait(1, i)

        @pl.when(jnp.logical_or(jnp.logical_not(is_last), i < 2))
        def _():
            f_compute(1, i, True)

        @pl.when(jnp.logical_and(is_last, i >= 2))
        def _():
            f_compute(1, i, False)

        @pl.when(jnp.logical_not(is_last))
        def _():
            f_hop(1, i).start()

        for copy in f_writes(1, i):
            copy.start()
        for k in range(2):
            @pl.when(jnp.logical_and(is_last, i == k))
            def _():
                remote, local = y_copies(k)
                for copy in remote:
                    copy.start()
                local.start()
        return carry

    lax.fori_loop(0, per, f_step_1, 0)

    def wt_reads():
        return (pltpu.make_async_copy(wide_hbm, wide.at[1], wt_rd.at[0]),
                pltpu.make_async_copy(tall_hbm, tall.at[1], wt_rd.at[1]))

    def e_copy(layer):
        return pltpu.make_async_copy(e_buf.at[layer], e_out.at[layer], e_wr.at[layer])

    def b_writes(v, j):
        slot = lax.rem(j, 2)
        turned = [pltpu.make_async_copy(
            tall_stage.at[slot, :, pl.ds(c * unit, unit)], at_out.at[v, pl.ds(c * part_f, part_f), rows_of(j)],
            at_wr.at[slot, c]) for c in range(per)]
        return [pltpu.make_async_copy(q_buf.at[slot], q_out.at[v, rows_of(j)], q_wr.at[slot]),
                pltpu.make_async_copy(wide_stage.at[slot, :, pl.ds(0, unit)], ht_out.at[v, :, rows_of(j)], ht_wr.at[slot])] + turned

    def b_hop(v, j):
        slot = lax.rem(j, 2)
        wrap = is_first.astype(jnp.int32)
        return pltpu.make_async_remote_copy(
            src_ref=b_send_buf.at[slot], dst_ref=e_buf.at[lax.rem(v + wrap, 2), rows_of(j)],
            send_sem=b_send.at[slot], recv_sem=b_recv.at[lax.rem((1 - v) * per + j + per * wrap, 2 * per)],
            device_id={'stage': prv}, device_id_type=MESH)

    def d_copies(i):
        src = b_send_buf.at[i]
        dst = dx_ref.at[pl.ds(i * unit, unit)]
        remote = [pltpu.make_async_remote_copy(
            src_ref=src, dst_ref=dst, send_sem=d_send.at[i, k - 1], recv_sem=d_recv.at[i],
            device_id={'stage': k}, device_id_type=MESH) for k in range(1, stages)]
        return remote, pltpu.make_async_copy(src, dst, d_loc.at[i])

    def hops(v):
        return jnp.logical_not(jnp.logical_and(is_first, v == 0))

    for copy in wt_reads():
        copy.start()

    def b_compute(v, j, full):
        slot = lax.rem(j, 2)
        e_in = e_buf[v, rows_of(j), :]
        for c in range(hidden // f_chunk):
            cols = pl.ds(c * f_chunk, f_chunk)
            d_act = jnp.dot(e_in, wide[1 - v, :, cols], preferred_element_type=jnp.float32)
            q_buf[slot, :, cols] = (slope_buf[rows_of(slot), cols] * d_act).astype(jnp.bfloat16)
        for c in range(per):
            tall_stage[slot, :, pl.ds(c * unit, unit)] = a_back[slot, :, pl.ds(c * part_f, part_f)].T
        wide_stage[slot, :, pl.ds(0, unit)] = h_buf[v, rows_of(j), :].T
        if full:
            delta = jnp.dot(q_buf[slot], tall[1 - v], preferred_element_type=jnp.float32)
            b_send_buf[slot] = (e_in.astype(jnp.float32) + delta).astype(jnp.bfloat16)

    def b_step(n, carry):
        v, j = 1 - n // per, lax.rem(n, per)
        for copy in b_reads(v, j):
            copy.wait()

        @pl.when(n == 1)
        def _():
            for i in range(per - 2, per):
                for copy in f_writes(1, i):
                    copy.wait()

        @pl.when(n == per)
        def _():
            for copy in wt_reads():
                copy.wait()
            e_copy(1).start()

        @pl.when(n >= 2)
        def _():
            back = n - 2
            for copy in b_writes(1 - back // per, lax.rem(back, per)):
                copy.wait()

        @pl.when(jnp.logical_and(n >= 2, hops(1 - (n - 2) // per)))
        def _():
            b_hop(1 - (n - 2) // per, lax.rem(n - 2, per)).wait_send()

        pltpu.make_async_copy(x_ref.at[pl.ds(0, unit)], e_buf.at[v, rows_of(j)], b_recv.at[n]).wait()

        @pl.when(n == 2 * per - 1)
        def _():
            e_copy(0).start()

        @pl.when(jnp.logical_or(hops(v), j < 2))
        def _():
            b_compute(v, j, True)

        @pl.when(jnp.logical_not(jnp.logical_or(hops(v), j < 2)))
        def _():
            b_compute(v, j, False)

        @pl.when(hops(v))
        def _():
            b_hop(v, j).start()

        for copy in b_writes(v, j):
            copy.start()

        @pl.when(n + 2 < 2 * per)
        def _():
            ahead = n + 2
            for copy in b_reads(1 - ahead // per, lax.rem(ahead, per)):
                copy.start()

        for k in range(2):
            @pl.when(jnp.logical_and(is_first, n == per + k))
            def _():
                remote, local = d_copies(k)
                for copy in remote:
                    copy.start()
                local.start()
        return carry

    lax.fori_loop(0, 2 * per, b_step, 0)
    for j in range(per - 2, per):
        for copy in b_writes(0, j):
            copy.wait()

    def share_done(src, dst, send_sem, recv_sem):
        for blk in range(1, replicas):
            for half in range(2):
                share_copy(src, dst, send_sem, recv_sem, blk, half).wait_send()

    @pl.when(is_first)
    def _():
        for k in range(2):
            remote, local = d_copies(k)
            for copy in remote:
                copy.wait_send()
            local.wait()
        share_done(x_ref, h_buf.at[0], x_send, f_recv)

    @pl.when(jnp.logical_not(is_first))
    def _():
        for j in range(per - 2, per):
            b_hop(0, j).wait_send()
        for k in range(2):
            pltpu.make_async_copy(b_send_buf.at[k], dx_ref.at[pl.ds(k * unit, unit)], d_recv.at[k]).wait()

    @pl.when(is_last)
    def _():
        for k in range(2):
            remote, local = y_copies(k)
            for copy in remote:
                copy.wait_send()
            local.wait()
        share_done(g_ref, e_buf.at[1], g_send, b_recv)

    @pl.when(jnp.logical_not(is_last))
    def _():
        for i in range(per - 2, per):
            f_hop(1, i).wait_send()
        for k in range(2):
            pltpu.make_async_copy(f_send_buf.at[k], y_ref.at[pl.ds(k * unit, unit)], y_recv.at[k]).wait()

    for layer in range(2):
        e_copy(layer).wait()


def run_chain(x, g, w_in, w_out, stages, replicas):
    rows, model = x.shape
    hidden = w_in.shape[-1]
    total = rows * replicas
    unit, per = rows // 2, 2 * replicas
    f_chunk = hidden // 4
    part_f = hidden // per
    any_spec = pl.BlockSpec(memory_space=pl.ANY)
    bf, f32 = jnp.bfloat16, jnp.float32
    dma = pltpu.SemaphoreType.DMA
    shape = jax.ShapeDtypeStruct
    return pl.pallas_call(
        functools.partial(chain_kernel, stages, replicas, f_chunk),
        out_shape=(shape((rows, model), bf), shape((rows, model), bf),
                   shape((2, model, total), bf), shape((2, total, model), bf),
                   shape((2, hidden, total), bf), shape((2, total, hidden), bf),
                   shape((2, total, hidden), bf), shape((2, total, hidden), f32), shape((model, hidden), bf), shape((hidden, model), bf)),
        in_specs=[any_spec] * 4,
        out_specs=(any_spec,) * 10,
        scratch_shapes=[
            pltpu.VMEM((2, total, model), bf), pltpu.VMEM((2, total, model), bf),
            pltpu.VMEM((2, model, hidden), bf), pltpu.VMEM((2, hidden, model), bf),
            pltpu.VMEM((4 * unit, hidden), f32), pltpu.VMEM((2, unit, hidden), bf), pltpu.VMEM((2, unit, hidden), bf), pltpu.VMEM((2, unit, hidden), bf),
            pltpu.VMEM((2, unit, model), bf), pltpu.VMEM((2, unit, model), bf),
            pltpu.VMEM((2, model, part_f), bf), pltpu.VMEM((2, part_f, model), bf),
            dma((2, 2)), dma((2, 2)), dma((2,)), dma((2 * per,)), dma((2 * per,)), dma((2,)), dma((2,)), dma((per,)), dma((per,)),
            dma((2,)), dma((2,)), dma((2,)), dma((2,)), dma((2,)), dma((2,)), dma((2, per)), dma((2,)),
            dma((2, stages - 1)), dma((2,)), dma((2,)), dma((2, stages - 1)), dma((2,)), dma((2,)),
        ],
        compiler_params=pltpu.CompilerParams(collective_id=0, has_side_effects=True, vmem_limit_bytes=VMEM_BYTES),
        name='chain',
    )(x, g, w_in, w_out)


def grad_kernel(ht_ref, q_ref, at_ref, e_ref, first_ref, second_ref):
    first_ref[0] = jnp.dot(ht_ref[0], q_ref[0], preferred_element_type=jnp.float32)
    second_ref[0] = jnp.dot(at_ref[0], e_ref[0], preferred_element_type=jnp.float32)


def run_grads(ht, q, at, e):
    layers, model, total = ht.shape
    hidden = at.shape[1]
    tile = hidden // 8
    whole = lambda v, i: (v, 0, 0)
    return pl.pallas_call(
        grad_kernel,
        grid=(layers, hidden // tile),
        out_shape=(jax.ShapeDtypeStruct((layers, model, hidden), jnp.float32),
                   jax.ShapeDtypeStruct((layers, hidden, model), jnp.float32)),
        in_specs=[pl.BlockSpec((1, model, total), whole), pl.BlockSpec((1, total, tile), lambda v, i: (v, 0, i)),
                  pl.BlockSpec((1, tile, total), lambda v, i: (v, i, 0)), pl.BlockSpec((1, total, model), whole)],
        out_specs=(pl.BlockSpec((1, model, tile), lambda v, i: (v, 0, i)),
                   pl.BlockSpec((1, tile, model), lambda v, i: (v, i, 0))),
        compiler_params=pltpu.CompilerParams(dimension_semantics=('arbitrary', 'arbitrary'), vmem_limit_bytes=60_000_000),
        name='grads',
    )(ht, q, at, e)


def solution(mesh):
    stages = mesh.shape['stage']
    replicas = mesh.shape['data']

    def local_fn(x, g, w_in, w_out):
        micro, tokens, model = x.shape
        y, dx, ht, e_all, at, q_all, *_ = run_chain(
            x.reshape(micro * tokens, model), g.reshape(micro * tokens, model), w_in, w_out, stages, replicas)
        grad_first, grad_second = run_grads(ht, q_all, at, e_all)
        return y.reshape(x.shape), dx.reshape(x.shape), grad_first[:, None], grad_second[:, None]

    spec_rows = P(('part', 'data'))
    spec_weights = P(None, 'stage')
    spec_grads = P('part', 'stage')
    return jax.shard_map(local_fn, mesh=mesh, in_specs=(spec_rows, spec_rows, spec_weights, spec_weights), out_specs=(spec_rows, spec_rows, spec_grads, spec_grads), check_vma=False)
```

```python
import functools
import math
import jax
import jax.numpy as jnp
from jax import lax
from jax.experimental import pallas as pl
from jax.experimental.pallas import tpu as pltpu
from jax.sharding import PartitionSpec as P

MESH = pl.DeviceIdType.MESH
VMEM_BYTES = 67_000_000
BLOCK_OF = (0, 1, 3, 2)
GELU_K0 = math.sqrt(2.0 / math.pi)
GELU_K1 = GELU_K0 * 0.044715


def gelu_pair(z):
    sq = z * z
    cdf = 0.5 * jnp.tanh(z * (GELU_K0 + GELU_K1 * sq)) + 0.5
    val = z * cdf
    slope = cdf + (val * (1.0 - cdf)) * (2.0 * GELU_K0 + 6.0 * GELU_K1 * sq)
    return val, slope


def chain_kernel(stages, replicas, f_chunk,
                 x_ref, g_ref, w_in_ref, w_out_ref,
                 y_ref, dx_ref, ht_out, e_out, at_out, q_out, a_hbm, slope_hbm, wide_hbm, tall_hbm,
                 h_buf, e_buf, wide, tall, slope_buf, a_buf, a_back, q_buf, f_send_buf, b_send_buf, wide_stage, tall_stage,
                 w_sem, wt_wr, wt_rd, f_recv, b_recv, f_send, b_send, x_send, g_send,
                 slope_wr, slope_rd, a_wr, a_rd, q_wr, ht_wr, at_wr, e_wr,
                 y_send, y_loc, y_recv, d_send, d_loc, d_recv):
    stage = lax.axis_index('stage')
    data = lax.axis_index('data')
    unit = x_ref.shape[0] // 2
    per = 2 * replicas
    hidden = wide.shape[2]
    part_f = hidden // per
    is_first = stage == 0
    is_last = stage == stages - 1
    nxt = lax.rem(stage + 1, stages)
    prv = lax.rem(stage + stages - 1, stages)

    def rows_of(i):
        return pl.ds(pl.multiple_of(i * unit, unit), unit)

    def weight_copies(layer):
        return (pltpu.make_async_copy(w_in_ref.at[layer, 0], wide.at[layer], w_sem.at[layer, 0]),
                pltpu.make_async_copy(w_out_ref.at[layer, 0], tall.at[layer], w_sem.at[layer, 1]))

    weight_copies(0)[0].start()

    barrier = pltpu.get_barrier_semaphore()
    for off in range(1, stages):
        pl.semaphore_signal(barrier, inc=1, device_id={'stage': lax.rem(stage + off, stages)}, device_id_type=MESH)
    for off in range(1, replicas):
        pl.semaphore_signal(barrier, inc=1, device_id={'data': lax.rem(data + off, replicas)}, device_id_type=MESH)
    pl.semaphore_wait(barrier, stages + replicas - 2)

    def share_copy(src, dst, send_sem, recv_sem, blk, half):
        slot = 2 * blk + half
        return pltpu.make_async_remote_copy(
            src_ref=src.at[pl.ds(half * unit, unit)], dst_ref=dst.at[pl.ds(slot * unit, unit)],
            send_sem=send_sem.at[slot], recv_sem=recv_sem.at[slot],
            device_id={'data': lax.rem(data + replicas - BLOCK_OF[blk], replicas)}, device_id_type=MESH)

    def share(src, dst, send_sem, recv_sem):
        for half in range(2):
            rows = pl.ds(half * unit, unit)
            pltpu.make_async_copy(src.at[rows], dst.at[rows], recv_sem.at[half]).start()
        for blk in range(1, replicas):
            for half in range(2):
                share_copy(src, dst, send_sem, recv_sem, blk, half).start()

    @pl.when(is_first)
    def _():
        share(x_ref, h_buf.at[0], x_send, f_recv)

    @pl.when(is_last)
    def _():
        share(g_ref, e_buf.at[1], g_send, b_recv)

    def f_hop(v, i):
        slot = lax.rem(i, 2)
        last = is_last.astype(jnp.int32)
        return pltpu.make_async_remote_copy(
            src_ref=f_send_buf.at[slot], dst_ref=h_buf.at[lax.rem(v + last, 2), rows_of(i)],
            send_sem=f_send.at[slot], recv_sem=f_recv.at[lax.rem(v * per + i + per * last, 2 * per)],
            device_id={'stage': nxt}, device_id_type=MESH)

    def y_copies(i):
        src = f_send_buf.at[i]
        dst = y_ref.at[pl.ds(i * unit, unit)]
        remote = [pltpu.make_async_remote_copy(
            src_ref=src, dst_ref=dst, send_sem=y_send.at[i, k], recv_sem=y_recv.at[i],
            device_id={'stage': k}, device_id_type=MESH) for k in range(stages - 1)]
        return remote, pltpu.make_async_copy(src, dst, y_loc.at[i])

    def f_writes(v, i):
        slot = lax.rem(i, 2)
        return (pltpu.make_async_copy(slope_buf.at[rows_of(2 + slot)], slope_hbm.at[v, rows_of(i)], slope_wr.at[slot]),
                pltpu.make_async_copy(a_buf.at[slot], a_hbm.at[v, rows_of(i)], a_wr.at[slot]))

    def wt_writes(i):
        slot = lax.rem(i, 2)
        return (pltpu.make_async_copy(wide_stage.at[slot], wide_hbm.at[:, pl.ds(pl.multiple_of(i * part_f, part_f), part_f)], wt_wr.at[slot, 0]),
                pltpu.make_async_copy(tall_stage.at[slot], tall_hbm.at[pl.ds(pl.multiple_of(i * part_f, part_f), part_f)], wt_wr.at[slot, 1]))

    def f_compute(v, i, full, before_second=None):
        slot = lax.rem(i, 2)
        h_in = h_buf[v, rows_of(i), :]
        for c in range(hidden // f_chunk):
            cols = pl.ds(c * f_chunk, f_chunk)
            z = jnp.dot(h_in, wide[v, :, cols], preferred_element_type=jnp.float32)
            val, slope = gelu_pair(z)
            slope_buf[rows_of(2 + slot), cols] = slope
            a_buf[slot, :, cols] = val.astype(jnp.bfloat16)
        if before_second is not None:
            before_second()
        strip = pl.ds(pl.multiple_of(i * part_f, part_f), part_f)
        if v == 0:
            wide_stage[slot] = tall[v, strip, :].T
            tall_stage[slot] = wide[v, :, strip].T
        else:
            wide[0, :, strip] = tall[v, strip, :].T
            tall[0, strip, :] = wide[v, :, strip].T
        if full:
            delta = jnp.dot(a_buf[slot], tall[v], preferred_element_type=jnp.float32)
            f_send_buf[slot] = (h_in.astype(jnp.float32) + delta).astype(jnp.bfloat16)

    def f_wait(v, i):
        pltpu.make_async_copy(x_ref.at[pl.ds(0, unit)], h_buf.at[v, rows_of(i)], f_recv.at[v * per + i]).wait()

    def second_weights():
        weight_copies(0)[1].wait()
        for copy in weight_copies(1):
            copy.start()

    weight_copies(0)[0].wait()
    weight_copies(0)[1].start()
    f_wait(0, 0)
    f_compute(0, 0, True, second_weights)
    f_hop(0, 0).start()
    for copy in f_writes(0, 0) + wt_writes(0):
        copy.start()

    def f_step_0(i, carry):
        @pl.when(i >= 2)
        def _():
            for copy in f_writes(0, i - 2) + wt_writes(i - 2):
                copy.wait()
            f_hop(0, i - 2).wait_send()

        f_wait(0, i)
        f_compute(0, i, True)
        f_hop(0, i).start()
        for copy in f_writes(0, i) + wt_writes(i):
            copy.start()
        return carry

    lax.fori_loop(1, per, f_step_0, 0)
    for copy in weight_copies(1):
        copy.wait()
    for i in range(per - 2, per):
        f_hop(0, i).wait_send()

    def b_reads(v, j):
        slot = lax.rem(j, 2)
        return (pltpu.make_async_copy(slope_hbm.at[v, rows_of(j)], slope_buf.at[rows_of(slot)], slope_rd.at[slot]),
                pltpu.make_async_copy(a_hbm.at[v, rows_of(j)], a_back.at[slot], a_rd.at[slot]))

    def f_step_1(i, carry):
        @pl.when(i < 2)
        def _():
            for copy in f_writes(0, per - 2 + i) + wt_writes(per - 2 + i):
                copy.wait()

        @pl.when(i >= 2)
        def _():
            for copy in f_writes(1, i - 2):
                copy.wait()

        for j in range(2):
            @pl.when(i == 2 + j)
            def _():
                for copy in b_reads(1, j):
                    copy.start()

        @pl.when(jnp.logical_and(i >= 2, jnp.logical_not(is_last)))
        def _():
            f_hop(1, i - 2).wait_send()

        f_wait(1, i)

        @pl.when(jnp.logical_or(jnp.logical_not(is_last), i < 2))
        def _():
            f_compute(1, i, True)

        @pl.when(jnp.logical_and(is_last, i >= 2))
        def _():
            f_compute(1, i, False)

        @pl.when(jnp.logical_not(is_last))
        def _():
            f_hop(1, i).start()

        for copy in f_writes(1, i):
            copy.start()
        for k in range(2):
            @pl.when(jnp.logical_and(is_last, i == k))
            def _():
                remote, local = y_copies(k)
                for copy in remote:
                    copy.start()
                local.start()
        return carry

    lax.fori_loop(0, per, f_step_1, 0)

    def wt_reads():
        return (pltpu.make_async_copy(wide_hbm, wide.at[1], wt_rd.at[0]),
                pltpu.make_async_copy(tall_hbm, tall.at[1], wt_rd.at[1]))

    def e_copy(layer):
        return pltpu.make_async_copy(e_buf.at[layer], e_out.at[layer], e_wr.at[layer])

    def b_writes(v, j):
        slot = lax.rem(j, 2)
        turned = [pltpu.make_async_copy(
            tall_stage.at[slot, :, pl.ds(c * unit, unit)], at_out.at[v, pl.ds(c * part_f, part_f), rows_of(j)],
            at_wr.at[slot, c]) for c in range(per)]
        return [pltpu.make_async_copy(q_buf.at[slot], q_out.at[v, rows_of(j)], q_wr.at[slot]),
                pltpu.make_async_copy(wide_stage.at[slot, :, pl.ds(0, unit)], ht_out.at[v, :, rows_of(j)], ht_wr.at[slot])] + turned

    def b_hop(v, j):
        slot = lax.rem(j, 2)
        wrap = is_first.astype(jnp.int32)
        return pltpu.make_async_remote_copy(
            src_ref=b_send_buf.at[slot], dst_ref=e_buf.at[lax.rem(v + wrap, 2), rows_of(j)],
            send_sem=b_send.at[slot], recv_sem=b_recv.at[lax.rem((1 - v) * per + j + per * wrap, 2 * per)],
            device_id={'stage': prv}, device_id_type=MESH)

    def d_copies(i):
        src = b_send_buf.at[i]
        dst = dx_ref.at[pl.ds(i * unit, unit)]
        remote = [pltpu.make_async_remote_copy(
            src_ref=src, dst_ref=dst, send_sem=d_send.at[i, k - 1], recv_sem=d_recv.at[i],
            device_id={'stage': k}, device_id_type=MESH) for k in range(1, stages)]
        return remote, pltpu.make_async_copy(src, dst, d_loc.at[i])

    def hops(v):
        return jnp.logical_not(jnp.logical_and(is_first, v == 0))

    for copy in wt_reads():
        copy.start()

    def b_compute(v, j, full):
        slot = lax.rem(j, 2)
        e_in = e_buf[v, rows_of(j), :]
        for c in range(hidden // f_chunk):
            cols = pl.ds(c * f_chunk, f_chunk)
            d_act = jnp.dot(e_in, wide[1 - v, :, cols], preferred_element_type=jnp.float32)
            q_buf[slot, :, cols] = (slope_buf[rows_of(slot), cols] * d_act).astype(jnp.bfloat16)
        for c in range(per):
            tall_stage[slot, :, pl.ds(c * unit, unit)] = a_back[slot, :, pl.ds(c * part_f, part_f)].T
        wide_stage[slot, :, pl.ds(0, unit)] = h_buf[v, rows_of(j), :].T
        if full:
            delta = jnp.dot(q_buf[slot], tall[1 - v], preferred_element_type=jnp.float32)
            b_send_buf[slot] = (e_in.astype(jnp.float32) + delta).astype(jnp.bfloat16)

    def b_step(n, carry):
        v, j = 1 - n // per, lax.rem(n, per)
        for copy in b_reads(v, j):
            copy.wait()

        @pl.when(n == 1)
        def _():
            for i in range(per - 2, per):
                for copy in f_writes(1, i):
                    copy.wait()

        @pl.when(n == per)
        def _():
            for copy in wt_reads():
                copy.wait()
            e_copy(1).start()

        @pl.when(n >= 2)
        def _():
            back = n - 2
            for copy in b_writes(1 - back // per, lax.rem(back, per)):
                copy.wait()

        @pl.when(jnp.logical_and(n >= 2, hops(1 - (n - 2) // per)))
        def _():
            b_hop(1 - (n - 2) // per, lax.rem(n - 2, per)).wait_send()

        pltpu.make_async_copy(x_ref.at[pl.ds(0, unit)], e_buf.at[v, rows_of(j)], b_recv.at[n]).wait()

        @pl.when(n == 2 * per - 1)
        def _():
            e_copy(0).start()

        @pl.when(jnp.logical_or(hops(v), j < 2))
        def _():
            b_compute(v, j, True)

        @pl.when(jnp.logical_not(jnp.logical_or(hops(v), j < 2)))
        def _():
            b_compute(v, j, False)

        @pl.when(hops(v))
        def _():
            b_hop(v, j).start()

        for copy in b_writes(v, j):
            copy.start()

        @pl.when(n + 2 < 2 * per)
        def _():
            ahead = n + 2
            for copy in b_reads(1 - ahead // per, lax.rem(ahead, per)):
                copy.start()

        for k in range(2):
            @pl.when(jnp.logical_and(is_first, n == per + k))
            def _():
                remote, local = d_copies(k)
                for copy in remote:
                    copy.start()
                local.start()
        return carry

    lax.fori_loop(0, 2 * per, b_step, 0)
    for j in range(per - 2, per):
        for copy in b_writes(0, j):
            copy.wait()

    def share_done(src, dst, send_sem, recv_sem):
        for blk in range(1, replicas):
            for half in range(2):
                share_copy(src, dst, send_sem, recv_sem, blk, half).wait_send()

    @pl.when(is_first)
    def _():
        for k in range(2):
            remote, local = d_copies(k)
            for copy in remote:
                copy.wait_send()
            local.wait()
        share_done(x_ref, h_buf.at[0], x_send, f_recv)

    @pl.when(jnp.logical_not(is_first))
    def _():
        for j in range(per - 2, per):
            b_hop(0, j).wait_send()
        for k in range(2):
            pltpu.make_async_copy(b_send_buf.at[k], dx_ref.at[pl.ds(k * unit, unit)], d_recv.at[k]).wait()

    @pl.when(is_last)
    def _():
        for k in range(2):
            remote, local = y_copies(k)
            for copy in remote:
                copy.wait_send()
            local.wait()
        share_done(g_ref, e_buf.at[1], g_send, b_recv)

    @pl.when(jnp.logical_not(is_last))
    def _():
        for i in range(per - 2, per):
            f_hop(1, i).wait_send()
        for k in range(2):
            pltpu.make_async_copy(f_send_buf.at[k], y_ref.at[pl.ds(k * unit, unit)], y_recv.at[k]).wait()

    for layer in range(2):
        e_copy(layer).wait()


def run_chain(x, g, w_in, w_out, stages, replicas):
    rows, model = x.shape
    hidden = w_in.shape[-1]
    total = rows * replicas
    unit, per = rows // 2, 2 * replicas
    f_chunk = hidden // 4
    part_f = hidden // per
    any_spec = pl.BlockSpec(memory_space=pl.ANY)
    bf, f32 = jnp.bfloat16, jnp.float32
    dma = pltpu.SemaphoreType.DMA
    shape = jax.ShapeDtypeStruct
    return pl.pallas_call(
        functools.partial(chain_kernel, stages, replicas, f_chunk),
        out_shape=(shape((rows, model), bf), shape((rows, model), bf),
                   shape((2, model, total), bf), shape((2, total, model), bf),
                   shape((2, hidden, total), bf), shape((2, total, hidden), bf),
                   shape((2, total, hidden), bf), shape((2, total, hidden), f32), shape((model, hidden), bf), shape((hidden, model), bf)),
        in_specs=[any_spec] * 4,
        out_specs=(any_spec,) * 10,
        scratch_shapes=[
            pltpu.VMEM((2, total, model), bf), pltpu.VMEM((2, total, model), bf),
            pltpu.VMEM((2, model, hidden), bf), pltpu.VMEM((2, hidden, model), bf),
            pltpu.VMEM((4 * unit, hidden), f32), pltpu.VMEM((2, unit, hidden), bf), pltpu.VMEM((2, unit, hidden), bf), pltpu.VMEM((2, unit, hidden), bf),
            pltpu.VMEM((2, unit, model), bf), pltpu.VMEM((2, unit, model), bf),
            pltpu.VMEM((2, model, part_f), bf), pltpu.VMEM((2, part_f, model), bf),
            dma((2, 2)), dma((2, 2)), dma((2,)), dma((2 * per,)), dma((2 * per,)), dma((2,)), dma((2,)), dma((per,)), dma((per,)),
            dma((2,)), dma((2,)), dma((2,)), dma((2,)), dma((2,)), dma((2,)), dma((2, per)), dma((2,)),
            dma((2, stages - 1)), dma((2,)), dma((2,)), dma((2, stages - 1)), dma((2,)), dma((2,)),
        ],
        compiler_params=pltpu.CompilerParams(collective_id=0, has_side_effects=True, vmem_limit_bytes=VMEM_BYTES),
        name='chain',
    )(x, g, w_in, w_out)


def grad_kernel(ht_ref, q_ref, at_ref, e_ref, y_ref, dx_ref, first_ref, second_ref, y_out, dx_out):
    y_out[...] = y_ref[...]
    dx_out[...] = dx_ref[...]
    first_ref[0] = jnp.dot(ht_ref[0], q_ref[0], preferred_element_type=jnp.float32)
    second_ref[0] = jnp.dot(at_ref[0], e_ref[0], preferred_element_type=jnp.float32)


def run_grads(ht, q, at, e, y, dx):
    layers, model, total = ht.shape
    hidden = at.shape[1]
    tile = hidden // 8
    rows = y.shape[0] // (layers * 8)
    few = pl.BlockSpec((rows, model), lambda v, i: (v * 8 + i, 0))
    whole = lambda v, i: (v, 0, 0)
    return pl.pallas_call(
        grad_kernel,
        grid=(layers, hidden // tile),
        out_shape=(jax.ShapeDtypeStruct((layers, model, hidden), jnp.float32),
                   jax.ShapeDtypeStruct((layers, hidden, model), jnp.float32),
                   jax.ShapeDtypeStruct(y.shape, y.dtype), jax.ShapeDtypeStruct(dx.shape, dx.dtype)),
        in_specs=[pl.BlockSpec((1, model, total), whole), pl.BlockSpec((1, total, tile), lambda v, i: (v, 0, i)),
                  pl.BlockSpec((1, tile, total), lambda v, i: (v, i, 0)), pl.BlockSpec((1, total, model), whole), few, few],
        out_specs=(pl.BlockSpec((1, model, tile), lambda v, i: (v, 0, i)),
                   pl.BlockSpec((1, tile, model), lambda v, i: (v, i, 0)), few, few),
        compiler_params=pltpu.CompilerParams(dimension_semantics=('arbitrary', 'arbitrary'), vmem_limit_bytes=60_000_000),
        name='grads',
    )(ht, q, at, e, y, dx)


def solution(mesh):
    stages = mesh.shape['stage']
    replicas = mesh.shape['data']

    def local_fn(x, g, w_in, w_out):
        micro, tokens, model = x.shape
        y, dx, ht, e_all, at, q_all, *_ = run_chain(
            x.reshape(micro * tokens, model), g.reshape(micro * tokens, model), w_in, w_out, stages, replicas)
        grad_first, grad_second, y, dx = run_grads(ht, q_all, at, e_all, y, dx)
        return y.reshape(x.shape), dx.reshape(x.shape), grad_first[:, None], grad_second[:, None]

    spec_rows = P(('part', 'data'))
    spec_weights = P(None, 'stage')
    spec_grads = P('part', 'stage')
    return jax.shard_map(local_fn, mesh=mesh, in_specs=(spec_rows, spec_rows, spec_weights, spec_weights), out_specs=(spec_rows, spec_rows, spec_grads, spec_grads), check_vma=False)
```
